32 devices in a mesh: seq: 8 (over z, x), head: 4 (over y, core).
Axes of the slice: x: 2, y: 2, z: 4, core: 2. Of those that a mesh axis runs over, the one named last changes fastest.
Arguments:
- query: bfloat16 [4096, 4096], P(('seq', 'head')), may hold values from -6 to 6
- key: bfloat16 [4096, 1024], P(('seq', 'head')), may hold values from -6 to 6
- value: bfloat16 [4096, 1024], P(('seq', 'head')), may hold values from -6 to 6
- out: bfloat16 [4096, 4096], P(('seq', 'head')), may hold values from -4 to 4
- output_gradient: bfloat16 [4096, 4096], P(('seq', 'head')), may hold values from -6 to 6
- log_sum_exp: float32 [4096, 32], P(('seq', 'head')), may hold values from 4 to 7
- segment_ids: int32 [4096], replicated, may hold values from 0 to 3, never falling along the last dimension, each value on 1 to 1536 neighbouring positions
Outputs:
- d_query: bfloat16 [4096, 4096], P(('seq', 'head'))
- key_gradient: bfloat16 [4096, 1024], P(('seq', 'head'))
- value_gradient: bfloat16 [4096, 1024], P(('seq', 'head'))
The draws below stay inside these ranges and needn't reach their ends.
Inputs may be any that keep to these rules, and one draw needn't show every extreme that they name: `segment_ids`: never falls along the positions; a document holds at most 1536 positions, and one holds exactly 1536.
All inputs are finite; a program needn't handle non-finite values.
Results may differ from the reference program's by a relative error of at most 0.0071.
Values may be sent and summed in bfloat16 or wider, within the bound.
No kernel may reach another device: no remote copies, remote signals or barrier semaphores. Data moves between devices by JAX's collectives and lax.ppermute only.
A program may use at most 128 MiB of HBM per device.

```python
import math
import jax
import jax.numpy as jnp
import numpy as np
from jax import lax

QUERY_HEADS = 32
KEY_VALUE_HEADS = 8
HEAD_SIZE = 128
TOK_DEV = 128
REACH = 3
PACKED_TOKENS = 4096
MOST = 1536
DOCS = 4
N_HEAD = 4


def block_levels(rng, shape, pieces, low, top_value):
    level, own = 1.0, jax.random.fold_in(rng, 6)
    for axis_at, shards_of in pieces:
        heights = jnp.exp(jax.random.uniform(jax.random.fold_in(own, axis_at), (shards_of,), jnp.float32, low / len(pieces), top_value / len(pieces)))
        level = level * jnp.repeat(heights, shape[axis_at] // shards_of).reshape([-1 if axis == axis_at else 1 for axis in range(len(shape))])
    return level


def split_up(number_of, total, most, slope):
    portions = [(1 << 20) // math.isqrt(rank ** slope) + 1 for rank in range(2, number_of + 1)]
    spare, counts = total - most - (number_of - 1), [1] * (number_of - 1)
    while spare > 0:
        movable = [i for i in range(number_of - 1) if counts[i] < most]
        pool, budget = sum([portions[i] for i in movable]), spare
        for i in movable:
            more = min(most - counts[i], max(1, budget * portions[i] // pool), spare)
            counts[i] = counts[i] + more
            spare = spare - more
    return np.array([most] + counts)


def uneven_parts(key, number_of, total, most, lean):
    if number_of == 2:
        one = jax.random.randint(key, (), max(1, total - most), min(most, total - 1) + 1)
        return jnp.stack([one, total - one])
    sizes = jnp.asarray(split_up(number_of, total, most, lean), jnp.int32)
    couples = (number_of - 1) // 2
    donor, sink = sizes[1:1 + 2 * couples:2], sizes[2:2 + 2 * couples:2]
    slack = jnp.minimum(donor - 1, most - sink)
    moved = jax.random.randint(jax.random.fold_in(key, 1), (couples,), 0, 1 << 20) % (slack + 1)
    sizes = sizes.at[1:1 + 2 * couples:2].set(donor - moved).at[2:2 + 2 * couples:2].set(sink + moved)
    return sizes[jax.random.permutation(jax.random.fold_in(key, 2), number_of)]


def noise(rng, shape, width, bound, cuts=(), kind=jnp.bfloat16):
    level = block_levels(rng, shape, cuts, -0.22, 0.18) if cuts else 1.0
    entries = jax.random.normal(rng, shape, jnp.float32) * width * level
    return jnp.minimum(jnp.maximum(entries, -bound), bound).astype(kind)


def setup_inputs(seed: int = 0) -> dict:
    streams_of = jax.random.split(jax.random.key(seed), 8)
    query = noise(streams_of[0], (PACKED_TOKENS, QUERY_HEADS * HEAD_SIZE), 1.0, 6.0, ((0, 32),))
    key = noise(streams_of[1], (PACKED_TOKENS, KEY_VALUE_HEADS * HEAD_SIZE), 1.0, 6.0, ((0, 32),))
    value = noise(streams_of[2], (PACKED_TOKENS, KEY_VALUE_HEADS * HEAD_SIZE), 1.0, 6.0, ((0, 32),))
    out = noise(streams_of[3], (PACKED_TOKENS, QUERY_HEADS * HEAD_SIZE), 0.5, 4.0, ((0, 32),))
    output_gradient = noise(streams_of[4], (PACKED_TOKENS, QUERY_HEADS * HEAD_SIZE), 1.0, 6.0, ((0, 32),))
    log_sum_exp = jnp.clip(4.0 + 3.0 * jax.random.uniform(streams_of[5], (PACKED_TOKENS, QUERY_HEADS), jnp.float32) ** block_levels(streams_of[5], (PACKED_TOKENS, QUERY_HEADS), ((0, 32),), -0.2, 0.2), 4.0, 7.0)
    segment_ids = jnp.searchsorted(jnp.cumsum(uneven_parts(streams_of[6], DOCS, PACKED_TOKENS, MOST, 2)), jnp.arange(PACKED_TOKENS), side="right").astype(jnp.int32)
    return {"query": query, "key": key, "value": value, "out": out, "output_gradient": output_gradient, "log_sum_exp": log_sum_exp, "segment_ids": segment_ids}


def rounded(values):
    return lax.optimization_barrier(values.astype(jnp.bfloat16)).astype(jnp.float32)

def reference(query, key, value, out, output_gradient, log_sum_exp, segment_ids):
    row_number = TOK_DEV * N_HEAD
    block_list = PACKED_TOKENS // row_number
    group_width = QUERY_HEADS // KEY_VALUE_HEADS
    score_scale = 1.0 / math.sqrt(HEAD_SIZE)
    padding_rows = REACH * row_number
    window_rows = (REACH + 1) * row_number
    query_total = query.astype(jnp.float32).reshape(block_list, row_number, KEY_VALUE_HEADS, group_width, HEAD_SIZE)
    gradient_total = output_gradient.astype(jnp.float32).reshape(block_list, row_number, KEY_VALUE_HEADS, group_width, HEAD_SIZE)
    output_total = out.astype(jnp.float32).reshape(block_list, row_number, KEY_VALUE_HEADS, group_width, HEAD_SIZE)
    delta_all = lax.optimization_barrier(jnp.sum(gradient_total * output_total, axis=4))
    log_sum_exp_total = log_sum_exp.astype(jnp.float32).reshape(block_list, row_number, KEY_VALUE_HEADS, group_width)
    key_padded = jnp.concatenate([jnp.zeros((padding_rows, KEY_VALUE_HEADS * HEAD_SIZE), jnp.float32), key.astype(jnp.float32)], axis=0).reshape(padding_rows + PACKED_TOKENS, KEY_VALUE_HEADS, HEAD_SIZE)
    value_padded = jnp.concatenate([jnp.zeros((padding_rows, KEY_VALUE_HEADS * HEAD_SIZE), jnp.float32), value.astype(jnp.float32)], axis=0).reshape(padding_rows + PACKED_TOKENS, KEY_VALUE_HEADS, HEAD_SIZE)
    seg_ids = segment_ids.astype(jnp.int32)
    seg_pad = jnp.concatenate([jnp.full((padding_rows,), -1, jnp.int32), seg_ids])
    query_offsets = jnp.arange(row_number, dtype=jnp.int32) + padding_rows
    key_offsets = jnp.arange(window_rows, dtype=jnp.int32)

    def block_step(accums, inputs):
        key_gradient_total, value_gradient_total = accums
        query_heads, grad_heads, delta_rows, lse_rows, index = inputs
        window_start = (index * row_number).astype(jnp.int32)
        key_block = lax.dynamic_slice_in_dim(key_padded, window_start, window_rows, 0)
        value_block = lax.dynamic_slice_in_dim(value_padded, window_start, window_rows, 0)
        seg_keys = lax.dynamic_slice_in_dim(seg_pad, window_start, window_rows, 0)
        seg_query = lax.dynamic_slice_in_dim(seg_ids, window_start, row_number, 0)
        allowed = (seg_query[:, None] == seg_keys[None, :]) & (key_offsets[None, :] <= query_offsets[:, None])
        lse_cols = lse_rows.transpose(1, 2, 0)[..., None]
        delta_cols = delta_rows.transpose(1, 2, 0)[..., None]
        scores = jnp.einsum('igmd,jgd->gmij', query_heads, key_block) * score_scale
        probs = jnp.exp(jnp.where(allowed, scores - lse_cols, -jnp.inf))
        probs_low = rounded(probs)
        dprobs = jnp.einsum('igmd,jgd->gmij', grad_heads, value_block)
        dscores = rounded(score_scale * probs * (dprobs - delta_cols))
        grad_query = jnp.einsum('gmij,jgd->igmd', dscores, key_block)
        grad_key = jnp.einsum('gmij,igmd->jgd', dscores, query_heads)
        grad_value = jnp.einsum('gmij,igmd->jgd', probs_low, grad_heads)
        key_gradient_total = lax.dynamic_update_slice_in_dim(key_gradient_total, lax.dynamic_slice_in_dim(key_gradient_total, window_start, window_rows, 0) + grad_key, window_start, 0)
        value_gradient_total = lax.dynamic_update_slice_in_dim(value_gradient_total, lax.dynamic_slice_in_dim(value_gradient_total, window_start, window_rows, 0) + grad_value, window_start, 0)
        return ((key_gradient_total, value_gradient_total), grad_query.astype(jnp.bfloat16))
    starting_totals = (jnp.zeros((padding_rows + PACKED_TOKENS, KEY_VALUE_HEADS, HEAD_SIZE), jnp.float32), jnp.zeros((padding_rows + PACKED_TOKENS, KEY_VALUE_HEADS, HEAD_SIZE), jnp.float32))
    indices = jnp.arange(block_list, dtype=jnp.int32)
    (key_gradient_total, value_gradient_total), grad_blocks = lax.scan(block_step, starting_totals, (query_total, gradient_total, delta_all, log_sum_exp_total, indices))
    d_query = grad_blocks.reshape(PACKED_TOKENS, QUERY_HEADS * HEAD_SIZE)
    key_gradient = key_gradient_total[padding_rows:].reshape(PACKED_TOKENS, KEY_VALUE_HEADS * HEAD_SIZE).astype(jnp.bfloat16)
    value_gradient = value_gradient_total[padding_rows:].reshape(PACKED_TOKENS, KEY_VALUE_HEADS * HEAD_SIZE).astype(jnp.bfloat16)
    return (d_query, key_gradient, value_gradient)
```

```python
import functools
import math

import jax
import jax.numpy as jnp
from jax import lax
from jax.experimental import pallas as pl
from jax.experimental.pallas import tpu as pltpu
from jax.sharding import Mesh, PartitionSpec as P

HEAD_SIZE = 128
LONGEST = 1536
TILE_Q = 256
TILE_K = 256
LOG2E = math.log2(math.e)
GROUP = ("inner", "head")


def dot(a, b, dims):
    return lax.dot_general(a, b, (dims, ((), ())), preferred_element_type=jnp.float32)


def tile_grads(qdo_ref, stat_ref, start_ref, kv_ref, dq_t, dkv, q0, k0, key_pos, query_pos, heads):
    d = HEAD_SIZE
    factor = LOG2E / math.sqrt(d)
    rows = pl.ds(q0, TILE_Q)
    keys = pl.ds(k0, TILE_K)
    k = kv_ref[keys, :d]
    v = kv_ref[keys, d:]
    k_t = k.T
    at = key_pos + lax.broadcasted_iota(jnp.int32, (TILE_K, TILE_Q), 0)
    last = query_pos + lax.broadcasted_iota(jnp.int32, (1, TILE_Q), 1)
    allowed = (at >= start_ref[:, rows]) & (at <= last)
    grad_k = jnp.zeros((TILE_K, d), jnp.float32)
    grad_v = jnp.zeros((TILE_K, d), jnp.float32)
    for h in range(heads):
        q = qdo_ref[rows, h * d : (h + 1) * d]
        e = qdo_ref[rows, (heads + h) * d : (heads + h + 1) * d]
        scores = dot(k, q, ((1,), (1,)))
        dprobs = dot(v, e, ((1,), (1,)))
        raised = jnp.where(allowed, scores * factor - stat_ref[h : h + 1, rows], -jnp.inf)
        probs = jnp.exp2(raised)
        ds = (probs * (dprobs - stat_ref[heads + h : heads + h + 1, rows])).astype(jnp.bfloat16)
        grad_v += dot(probs.astype(jnp.bfloat16), e, ((1,), (0,)))
        grad_k += dot(ds, q, ((1,), (0,)))
        dq_t[h, :, rows] += dot(k_t, ds, ((1,), (0,)))
    dkv[keys, :d] += grad_k
    dkv[keys, d:] += grad_v


def far_kernel(low_ref, qdo_ref, stat_ref, start_ref, kv_ref, dq_t, dkv_out, dkv):
    heads, _, rows = dq_t.shape
    window = kv_ref.shape[0]
    dq_t[...] = jnp.zeros_like(dq_t)
    dkv[...] = jnp.zeros_like(dkv)

    def per_query(t, _):
        q0 = pl.multiple_of(t * TILE_Q, TILE_Q)

        def per_key(j, _):
            k0 = pl.multiple_of(j * TILE_K, TILE_K)
            tile_grads(qdo_ref, stat_ref, start_ref, kv_ref, dq_t, dkv, q0, k0, k0, window + q0, heads)
            return 0

        return lax.fori_loop(jnp.minimum(low_ref[t] // TILE_K, window // TILE_K), window // TILE_K, per_key, 0)

    lax.fori_loop(0, rows // TILE_Q, per_query, 0)
    scale = 1.0 / math.sqrt(HEAD_SIZE)
    dkv_out[:, :HEAD_SIZE] = (dkv[:, :HEAD_SIZE] * scale).astype(dkv_out.dtype)
    dkv_out[:, HEAD_SIZE:] = dkv[:, HEAD_SIZE:].astype(dkv_out.dtype)


def near_kernel(window, low_ref, qdo_ref, stat_ref, start_ref, kv_ref, dq_far, dq_out, dkv, dq_t):
    heads, d, rows = dq_far.shape
    dq_t[...] = dq_far[...]
    dkv[...] = jnp.zeros_like(dkv)
    scale = 1.0 / math.sqrt(HEAD_SIZE)

    def per_query(t, _):
        q0 = pl.multiple_of(t * TILE_Q, TILE_Q)

        def per_key(j, _):
            k0 = pl.multiple_of(j * TILE_K, TILE_K)
            tile_grads(
                qdo_ref, stat_ref, start_ref, kv_ref, dq_t, dkv, q0, k0, window + k0, window + q0, heads
            )
            return 0

        first = jnp.maximum(low_ref[t] - window, 0) // TILE_K
        lax.fori_loop(first, (q0 + TILE_Q) // TILE_K, per_key, 0)
        for h in range(heads):
            done = dq_t[h, :, pl.ds(q0, TILE_Q)] * scale
            dq_out[pl.ds(q0, TILE_Q), h * d : (h + 1) * d] = done.T.astype(dq_out.dtype)
        return 0

    lax.fori_loop(0, rows // TILE_Q, per_query, 0)
    dkv[:, :HEAD_SIZE] = dkv[:, :HEAD_SIZE] * scale


def shards(query, key, value, out, output_gradient, log_sum_exp, segment_ids):
    d = HEAD_SIZE
    tokens = query.shape[0]
    parts = lax.axis_size(GROUP)
    outers = lax.axis_size("outer")
    rows = tokens * parts
    heads = query.shape[1] // key.shape[1]
    window = LONGEST
    place = lax.axis_index("outer")

    kv = jnp.concatenate(
        [key.reshape(tokens, parts, d), value.reshape(tokens, parts, d)], axis=2
    ).transpose(1, 0, 2)
    kv = lax.all_to_all(kv, GROUP, 0, 0).reshape(rows, 2 * d)
    delta = jnp.sum(
        (output_gradient.astype(jnp.float32) * out.astype(jnp.float32)).reshape(tokens, -1, d), axis=2
    )
    stat = jnp.concatenate(
        [(log_sum_exp * LOG2E).reshape(tokens, parts, heads), delta.reshape(tokens, parts, heads)], axis=2
    ).transpose(1, 2, 0)
    stat = lax.all_to_all(stat, GROUP, 0, 0).transpose(1, 0, 2).reshape(2 * heads, rows)
    qdo = jnp.concatenate(
        [query.reshape(tokens, parts, heads * d), output_gradient.reshape(tokens, parts, heads * d)], axis=2
    ).transpose(1, 0, 2)
    qdo = lax.all_to_all(qdo, GROUP, 0, 0).reshape(rows, 2 * heads * d)

    steps = -(-window // rows)
    sizes = [min(rows, window - by * rows) for by in range(steps)]
    arrived = [
        lax.ppermute(kv[rows - sizes[by - 1] :], "outer", [(i, i + by) for i in range(outers - by)])
        for by in range(1, steps + 1)
    ]
    kv_far = jnp.concatenate(arrived[::-1], axis=0)

    padded = jnp.concatenate([jnp.full((window,), -1, segment_ids.dtype), segment_ids])
    seg_keys = lax.dynamic_slice_in_dim(padded, place * rows, window + rows, 0)
    seg_query = seg_keys[window:]
    start = jnp.sum((seg_keys[:, None] < seg_query[None, :]).astype(jnp.int32), axis=0)
    low = start[::TILE_Q]
    start = start[None, :]

    smem = pl.BlockSpec(memory_space=pltpu.SMEM)
    vmem = pl.BlockSpec(memory_space=pltpu.VMEM)
    flops = 10 * rows * d * heads
    dq_far, dkv_far = pl.pallas_call(
        far_kernel,
        out_shape=(
            jax.ShapeDtypeStruct((heads, d, rows), jnp.float32),
            jax.ShapeDtypeStruct((window, 2 * d), jnp.bfloat16),
        ),
        in_specs=[smem] + [vmem] * 4,
        out_specs=(vmem, vmem),
        scratch_shapes=[pltpu.VMEM((window, 2 * d), jnp.float32)],
        cost_estimate=pl.CostEstimate(flops=flops * 1024, bytes_accessed=1 << 22, transcendentals=0),
        name="far_grads",
    )(low, qdo, stat, start, kv_far)
    returned = []
    at = window
    for by in range(1, steps + 1):
        at -= sizes[by - 1]
        returned.append(
            lax.ppermute(
                dkv_far[at : at + sizes[by - 1]], "outer", [(i + by, i) for i in range(outers - by)]
            )
        )
    dq, dkv = pl.pallas_call(
        functools.partial(near_kernel, window),
        out_shape=(
            jax.ShapeDtypeStruct((rows, heads * d), jnp.bfloat16),
            jax.ShapeDtypeStruct((rows, 2 * d), jnp.float32),
        ),
        in_specs=[smem] + [vmem] * 5,
        out_specs=(vmem, vmem),
        scratch_shapes=[pltpu.VMEM((heads, d, rows), jnp.float32)],
        cost_estimate=pl.CostEstimate(flops=flops * 512, bytes_accessed=1 << 22, transcendentals=0),
        name="near_grads",
    )(low, qdo, stat, start, kv, dq_far)
    dq = lax.all_to_all(dq.reshape(parts, tokens, heads * d), GROUP, 0, 0)
    for by in range(1, steps + 1):
        part = returned[by - 1].astype(jnp.float32)
        dkv = dkv + jnp.pad(part, ((rows - sizes[by - 1], 0), (0, 0)))
    dkv = lax.all_to_all(dkv.astype(jnp.bfloat16).reshape(parts, tokens, 2 * d), GROUP, 0, 0)
    dkv = dkv.transpose(1, 0, 2)
    return (
        dq.transpose(1, 0, 2).reshape(tokens, -1),
        dkv[:, :, :d].reshape(tokens, -1),
        dkv[:, :, d:].reshape(tokens, -1),
    )


def solution(mesh):
    head = mesh.shape["head"]
    seq = mesh.shape["seq"]

    def run(query, key, value, out, output_gradient, log_sum_exp, segment_ids):
        inner = key.shape[1] // HEAD_SIZE // head
        finer = Mesh(mesh.devices.reshape(seq // inner, inner, head), ("outer", "inner", "head"))
        rows = P(("outer", "inner", "head"), None)
        return jax.shard_map(
            shards,
            mesh=finer,
            in_specs=(rows,) * 6 + (P(),),
            out_specs=(rows,) * 3,
            check_vma=False,
        )(query, key, value, out, output_gradient, log_sum_exp, segment_ids)

    return run
```

```python
import functools
import math

import jax
import jax.numpy as jnp
from jax import lax
from jax.experimental import pallas as pl
from jax.experimental.pallas import tpu as pltpu
from jax.sharding import Mesh, PartitionSpec as P


HEAD_SIZE = 128
LONGEST = 1536
TILE_Q = 256
TILE_K = 256
LOG2E = math.log2(math.e)
GROUP = ("inner", "head")


def dot(a, b, dims):
    return lax.dot_general(a, b, (dims, ((), ())), preferred_element_type=jnp.float32)


def tile_grads(get, stat_ref, start_ref, kv_ref, dq_t, dkv, q0, k0, key_pos, query_pos):
    d = HEAD_SIZE
    factor = LOG2E / math.sqrt(d)
    heads = len(get)
    rows = pl.ds(q0, TILE_Q)
    keys = pl.ds(k0, TILE_K)
    k = kv_ref[keys, :d]
    v = kv_ref[keys, d:]
    k_t = k.T
    at = key_pos + lax.broadcasted_iota(jnp.int32, (TILE_K, TILE_Q), 0)
    last = query_pos + lax.broadcasted_iota(jnp.int32, (1, TILE_Q), 1)
    allowed = (at >= start_ref[:, rows]) & (at <= last)
    grad_k = jnp.zeros((TILE_K, d), jnp.float32)
    grad_v = jnp.zeros((TILE_K, d), jnp.float32)
    for h in range(heads):
        q, e = get[h](q0)
        scores = dot(k, q, ((1,), (1,)))
        dprobs = dot(v, e, ((1,), (1,)))
        raised = jnp.where(allowed, scores * factor - stat_ref[2 * h : 2 * h + 1, rows], -jnp.inf)
        probs = jnp.exp2(raised)
        ds = (probs * (dprobs - stat_ref[2 * h + 1 : 2 * h + 2, rows])).astype(jnp.bfloat16)
        grad_v += dot(probs.astype(jnp.bfloat16), e, ((1,), (0,)))
        grad_k += dot(ds, q, ((1,), (0,)))
        dq_t[h, :, rows] += dot(k_t, ds, ((1,), (0,)))
    dkv[keys, :d] += grad_k
    dkv[keys, d:] += grad_v


def getters(bulk_refs, tokens):
    d = HEAD_SIZE
    get = []
    for ref in bulk_refs:
        heads = ref.shape[2] // (2 * d)
        for h in range(heads):

            def one(q0, ref=ref, h=h, heads=heads):
                chunks = pl.ds(q0 // tokens, TILE_Q // tokens)
                return tuple(
                    ref[chunks, :tokens, (n * heads + h) * d : (n * heads + h + 1) * d].reshape(TILE_Q, d)
                    for n in range(2)
                )

            get.append(one)
    return get


def sweep(get, low_ref, stat_ref, start_ref, kv_ref, dq_t, dkv, base, window, finish):
    rows = dq_t.shape[2]
    keys = kv_ref.shape[0]

    def per_query(t, _):
        q0 = pl.multiple_of(t * TILE_Q, TILE_Q)

        def per_key(j, _):
            k0 = pl.multiple_of(j * TILE_K, TILE_K)
            tile_grads(get, stat_ref, start_ref, kv_ref, dq_t, dkv, q0, k0, base + k0, window + q0)
            return 0

        first = jnp.clip(low_ref[t] - base, 0, keys) // TILE_K
        end = jnp.minimum(window + q0 + TILE_Q - base, keys) // TILE_K
        lax.fori_loop(first, end, per_key, 0)
        finish(q0)
        return 0

    lax.fori_loop(0, rows // TILE_Q, per_query, 0)


def write_dq(dq_t, heads, dq_out, q0):
    d = HEAD_SIZE
    scale = 1.0 / math.sqrt(d)
    for n, h in enumerate(heads):
        done = dq_t[h, :, pl.ds(q0, TILE_Q)] * scale
        dq_out[pl.ds(q0, TILE_Q), n * d : (n + 1) * d] = done.T.astype(dq_out.dtype)


def early_kernel(tokens, window, low_ref, bulk_a, stat_ref, start_ref, kv_ref, dq_t, dkv):
    dq_t[...] = jnp.zeros_like(dq_t)
    dkv[...] = jnp.zeros_like(dkv)
    get = getters([bulk_a], tokens)
    sweep(get, low_ref, stat_ref, start_ref, kv_ref, dq_t, dkv, window, window, lambda q0: None)


def far_kernel(
    tokens, low_ref, bulk_a, bulk_b, stat_ref, start_ref, kv_ref, dq_near, dq_out, dq_rest, dkv_out, dq_t, dkv
):
    d = HEAD_SIZE
    half = dq_near.shape[0]
    heads = dq_t.shape[0]
    dq_t[:half] = dq_near[...]
    dq_t[half:] = jnp.zeros_like(dq_rest)
    dkv[...] = jnp.zeros_like(dkv)
    get = getters([bulk_a, bulk_b], tokens)

    def finish(q0):
        write_dq(dq_t, range(half), dq_out, q0)

    sweep(get, low_ref, stat_ref, start_ref, kv_ref, dq_t, dkv, 0, kv_ref.shape[0], finish)
    dq_rest[...] = dq_t[half:heads]
    dkv_out[:, :d] = (dkv[:, :d] * (1.0 / math.sqrt(d))).astype(dkv_out.dtype)
    dkv_out[:, d:] = dkv[:, d:].astype(dkv_out.dtype)


def late_kernel(
    tokens, window, low_ref, bulk_b, stat_ref, start_ref, kv_ref, dq_far, dkv_near, dq_out, dkv, dq_t
):
    dq_t[...] = dq_far[...]
    dkv[...] = dkv_near[...]
    get = getters([bulk_b], tokens)

    def finish(q0):
        write_dq(dq_t, range(dq_t.shape[0]), dq_out, q0)

    sweep(get, low_ref, stat_ref, start_ref, kv_ref, dq_t, dkv, window, window, finish)
    dkv[:, :HEAD_SIZE] = dkv[:, :HEAD_SIZE] * (1.0 / math.sqrt(HEAD_SIZE))


def pieces_of(x):
    first = lax.reduce_precision(x, 8, 7)
    second = lax.reduce_precision(x - first, 8, 7)
    return [first, second, x - first - second]


def packed(query, grad, stat, parts):
    _, _, wide = query.shape
    both = jnp.concatenate([query, grad], axis=2).transpose(1, 0, 2)
    tail = jnp.stack(pieces_of(stat), axis=1).reshape(parts, -1, 2 * wide).astype(jnp.bfloat16)
    pad = -tail.shape[1] % 8
    return jnp.concatenate([both, jnp.pad(tail, ((0, 0), (0, pad), (0, 0)))], axis=1)


def unpacked_stat(bulk, tokens, lines):
    parts, _, wide = bulk.shape
    used = 3 * lines * tokens // wide
    tail = bulk[:, tokens : tokens + used].astype(jnp.float32).reshape(parts, 3, lines, tokens)
    stat = tail[:, 0] + tail[:, 1] + tail[:, 2]
    return stat.transpose(1, 0, 2).reshape(lines, parts * tokens)


def whole(query, key, value, out, output_gradient, log_sum_exp, segment_ids):
    d = HEAD_SIZE
    tokens = query.shape[0]
    parts = lax.axis_size(GROUP)
    outers = lax.axis_size("outer")
    rows = tokens * parts
    heads = query.shape[1] // key.shape[1]
    half = heads // 2
    window = LONGEST
    place = lax.axis_index("outer")

    kv = jnp.concatenate(
        [key.reshape(tokens, parts, d), value.reshape(tokens, parts, d)], axis=2
    ).transpose(1, 0, 2)
    kv = lax.all_to_all(kv, GROUP, 0, 0).reshape(rows, 2 * d)
    delta = jnp.sum(
        (output_gradient.astype(jnp.float32) * out.astype(jnp.float32)).reshape(tokens, -1, d), axis=2
    )
    stat = jnp.stack([log_sum_exp * LOG2E, delta], axis=2).reshape(tokens, parts, 2 * heads).transpose(1, 2, 0)
    query_heads = query.reshape(tokens, parts, heads * d)
    grad_heads = output_gradient.reshape(tokens, parts, heads * d)
    bulk = []
    for n in range(2):
        cut = slice(n * half * d, (n + 1) * half * d)
        sent = packed(
            query_heads[:, :, cut], grad_heads[:, :, cut], stat[:, 2 * half * n : 2 * half * (n + 1)], parts
        )
        bulk.append(lax.all_to_all(sent, GROUP, 0, 0))
    stats = [unpacked_stat(b, tokens, 2 * half) for b in bulk]

    steps = -(-window // rows)
    sizes = [min(rows, window - by * rows) for by in range(steps)]
    arrived = []
    for by in range(1, steps + 1):
        arrived.append(
            lax.ppermute(kv[rows - sizes[by - 1] :], "outer", [(i, i + by) for i in range(outers - by)])
        )
    kv_far = jnp.concatenate(arrived[::-1], axis=0)

    padded = jnp.concatenate([jnp.full((window,), -1, segment_ids.dtype), segment_ids])
    seg_keys = lax.dynamic_slice_in_dim(padded, place * rows, window + rows, 0)
    seg_query = seg_keys[window:]
    start = jnp.sum((seg_keys[:, None] < seg_query[None, :]).astype(jnp.int32), axis=0)
    low = start[::TILE_Q]
    start = start[None, :]

    smem = pl.BlockSpec(memory_space=pltpu.SMEM)
    vmem = pl.BlockSpec(memory_space=pltpu.VMEM)
    flops = 10 * rows * d * half * 512
    dq_shape = jax.ShapeDtypeStruct((half, d, rows), jnp.float32)
    dq_done = jax.ShapeDtypeStruct((rows, half * d), jnp.bfloat16)
    dkv_shape = jax.ShapeDtypeStruct((rows, 2 * d), jnp.float32)

    def call(kernel, out_shape, scratch, work, *operands):
        return pl.pallas_call(
            kernel,
            out_shape=out_shape,
            in_specs=[smem] + [vmem] * (len(operands) - 1),
            out_specs=(vmem,) * len(out_shape),
            scratch_shapes=scratch,
            cost_estimate=pl.CostEstimate(flops=work, bytes_accessed=1 << 22, transcendentals=0),
        )(*operands)

    dq_near, dkv_near = call(
        functools.partial(early_kernel, tokens, window),
        (dq_shape, dkv_shape),
        [],
        flops,
        *(low, bulk[0], stats[0], start, kv),
    )
    dq_a, dq_far, dkv_far = call(
        functools.partial(far_kernel, tokens),
        (dq_done, dq_shape, jax.ShapeDtypeStruct((window, 2 * d), jnp.bfloat16)),
        [pltpu.VMEM((heads, d, rows), jnp.float32), pltpu.VMEM((window, 2 * d), jnp.float32)],
        4 * flops,
        *(low, bulk[0], bulk[1], jnp.concatenate(stats, axis=0), start, kv_far, dq_near),
    )
    returned = []
    at = window
    for by in range(1, steps + 1):
        at -= sizes[by - 1]
        returned.append(
            lax.ppermute(
                dkv_far[at : at + sizes[by - 1]], "outer", [(i + by, i) for i in range(outers - by)]
            )
        )
    dq_a = lax.all_to_all(dq_a.reshape(parts, tokens, half * d), GROUP, 0, 0)
    dq_b, dkv = call(
        functools.partial(late_kernel, tokens, window),
        (dq_done, dkv_shape),
        [pltpu.VMEM((half, d, rows), jnp.float32)],
        flops,
        *(low, bulk[1], stats[1], start, kv, dq_far, dkv_near),
    )
    dq_b = lax.all_to_all(dq_b.reshape(parts, tokens, half * d), GROUP, 0, 0)
    for by in range(1, steps + 1):
        part = returned[by - 1].astype(jnp.float32)
        dkv = dkv + jnp.pad(part, ((rows - sizes[by - 1], 0), (0, 0)))
    dkv = lax.all_to_all(dkv.astype(jnp.bfloat16).reshape(parts, tokens, 2 * d), GROUP, 0, 0)
    dkv = dkv.transpose(1, 0, 2)
    return (
        jnp.concatenate([dq_a, dq_b], axis=2).transpose(1, 0, 2).reshape(tokens, -1),
        dkv[:, :, :d].reshape(tokens, -1),
        dkv[:, :, d:].reshape(tokens, -1),
    )


def solution(mesh):
    head = mesh.shape["head"]
    seq = mesh.shape["seq"]

    def run(query, key, value, out, output_gradient, log_sum_exp, segment_ids):
        inner = key.shape[1] // HEAD_SIZE // head
        finer = Mesh(mesh.devices.reshape(seq // inner, inner, head), ("outer", "inner", "head"))
        rows = P(("outer", "inner", "head"), None)
        return jax.shard_map(
            whole,
            mesh=finer,
            in_specs=(rows,) * 6 + (P(),),
            out_specs=(rows,) * 3,
            check_vma=False,
        )(query, key, value, out, output_gradient, log_sum_exp, segment_ids)

    return run
```

```python
import functools
import math

import jax
import jax.numpy as jnp
from jax import lax
from jax.experimental import pallas as pl
from jax.experimental.pallas import tpu as pltpu
from jax.sharding import Mesh, PartitionSpec as P


HEAD_SIZE = 128
LONGEST = 1536
TILE_Q = 256
TILE_K = 256
LOG2E = math.log2(math.e)
GROUP = ("inner", "head")


def dot(a, b, dims):
    return lax.dot_general(a, b, (dims, ((), ())), preferred_element_type=jnp.float32)


def tile_grads(get, stat_ref, start_ref, kv_ref, dq_t, dkv, q0, k0, key_pos, query_pos):
    d = HEAD_SIZE
    factor = LOG2E / math.sqrt(d)
    heads = len(get)
    rows = pl.ds(q0, TILE_Q)
    keys = pl.ds(k0, TILE_K)
    k = kv_ref[keys, :d]
    v = kv_ref[keys, d:]
    k_t = k.T
    at = key_pos + lax.broadcasted_iota(jnp.int32, (TILE_K, TILE_Q), 0)
    last = query_pos + lax.broadcasted_iota(jnp.int32, (1, TILE_Q), 1)
    allowed = (at >= start_ref[:, rows]) & (at <= last)
    grad_k = jnp.zeros((TILE_K, d), jnp.float32)
    grad_v = jnp.zeros((TILE_K, d), jnp.float32)
    for h in range(heads):
        q, e = get[h](q0)
        scores = dot(k, q, ((1,), (1,)))
        dprobs = dot(v, e, ((1,), (1,)))
        raised = jnp.where(allowed, scores * factor - stat_ref[2 * h : 2 * h + 1, rows], -jnp.inf)
        probs = jnp.exp2(raised)
        ds = (probs * (dprobs - stat_ref[2 * h + 1 : 2 * h + 2, rows])).astype(jnp.bfloat16)
        grad_v += dot(probs.astype(jnp.bfloat16), e, ((1,), (0,)))
        grad_k += dot(ds, q, ((1,), (0,)))
        dq_t[h, :, rows] += dot(k_t, ds, ((1,), (0,)))
    dkv[keys, :d] += grad_k
    dkv[keys, d:] += grad_v


def getters(bulk_refs, tokens):
    d = HEAD_SIZE
    get = []
    for ref in bulk_refs:
        heads = ref.shape[2] // (2 * d)
        for h in range(heads):

            def one(q0, ref=ref, h=h, heads=heads):
                chunks = pl.ds(q0 // tokens, TILE_Q // tokens)
                return tuple(
                    ref[chunks, :tokens, (n * heads + h) * d : (n * heads + h + 1) * d].reshape(TILE_Q, d)
                    for n in range(2)
                )

            get.append(one)
    return get


def sweep(get, low_ref, stat_ref, start_ref, kv_ref, dq_t, dkv, base, window, finish):
    rows = dq_t.shape[2]
    keys = kv_ref.shape[0]

    def per_query(t, _):
        q0 = pl.multiple_of(t * TILE_Q, TILE_Q)

        def per_key(j, _):
            k0 = pl.multiple_of(j * TILE_K, TILE_K)
            tile_grads(get, stat_ref, start_ref, kv_ref, dq_t, dkv, q0, k0, base + k0, window + q0)
            return 0

        first = jnp.clip(low_ref[t] - base, 0, keys) // TILE_K
        end = jnp.minimum(window + q0 + TILE_Q - base, keys) // TILE_K
        lax.fori_loop(first, end, per_key, 0)
        finish(q0)
        return 0

    lax.fori_loop(0, rows // TILE_Q, per_query, 0)


def write_dq(dq_t, heads, dq_out, q0):
    d = HEAD_SIZE
    scale = 1.0 / math.sqrt(d)
    for n, h in enumerate(heads):
        done = dq_t[h, :, pl.ds(q0, TILE_Q)] * scale
        dq_out[pl.ds(q0, TILE_Q), n * d : (n + 1) * d] = done.T.astype(dq_out.dtype)


def early_kernel(tokens, window, low_ref, bulk_a, stat_ref, start_ref, kv_ref, dq_t, dkv):
    dq_t[...] = jnp.zeros_like(dq_t)
    dkv[...] = jnp.zeros_like(dkv)
    get = getters([bulk_a], tokens)
    sweep(get, low_ref, stat_ref, start_ref, kv_ref, dq_t, dkv, window, window, lambda q0: None)


def far_kernel(tokens, steps, low_ref, bulk_a, bulk_b, stat_ref, start_ref, *refs):
    d = HEAD_SIZE
    kv_parts, refs = refs[:steps], refs[steps:]
    dq_near, dq_out, dq_rest, refs = refs[0], refs[1], refs[2], refs[3:]
    dkv_parts, (dq_t, dkv, kv_all) = refs[:steps], refs[steps:]
    half = dq_near.shape[0]
    heads = dq_t.shape[0]
    window = kv_all.shape[0]
    dq_t[:half] = dq_near[...]
    dq_t[half:] = jnp.zeros_like(dq_rest)
    dkv[...] = jnp.zeros_like(dkv)
    at = window
    for part in kv_parts:
        at -= part.shape[0]
        kv_all[at : at + part.shape[0], :] = part[...]
    get = getters([bulk_a, bulk_b], tokens)

    def finish(q0):
        write_dq(dq_t, range(half), dq_out, q0)

    sweep(get, low_ref, stat_ref, start_ref, kv_all, dq_t, dkv, 0, window, finish)
    dq_rest[...] = dq_t[half:heads]
    at = window
    for part in dkv_parts:
        at -= part.shape[0]
        cut = slice(at, at + part.shape[0])
        part[:, :d] = (dkv[cut, :d] * (1.0 / math.sqrt(d))).astype(part.dtype)
        part[:, d:] = dkv[cut, d:].astype(part.dtype)


def late_kernel(
    tokens, window, low_ref, bulk_b, stat_ref, start_ref, kv_ref, dq_far, dkv_near, dq_out, dkv, dq_t
):
    dq_t[...] = dq_far[...]
    dkv[...] = dkv_near[...]
    get = getters([bulk_b], tokens)

    def finish(q0):
        write_dq(dq_t, range(dq_t.shape[0]), dq_out, q0)

    sweep(get, low_ref, stat_ref, start_ref, kv_ref, dq_t, dkv, window, window, finish)
    dkv[:, :HEAD_SIZE] = dkv[:, :HEAD_SIZE] * (1.0 / math.sqrt(HEAD_SIZE))


def pieces_of(x):
    first = lax.reduce_precision(x, 8, 7)
    second = lax.reduce_precision(x - first, 8, 7)
    return [first, second, x - first - second]


def packed(query, grad, stat, parts):
    _, _, wide = query.shape
    both = jnp.concatenate([query, grad], axis=2).transpose(1, 0, 2)
    tail = jnp.stack(pieces_of(stat), axis=1).reshape(parts, -1, 2 * wide).astype(jnp.bfloat16)
    pad = -tail.shape[1] % 8
    return jnp.concatenate([both, jnp.pad(tail, ((0, 0), (0, pad), (0, 0)))], axis=1)


def unpacked_stat(bulk, tokens, lines):
    parts, _, wide = bulk.shape
    used = 3 * lines * tokens // wide
    tail = bulk[:, tokens : tokens + used].astype(jnp.float32).reshape(parts, 3, lines, tokens)
    stat = tail[:, 0] + tail[:, 1] + tail[:, 2]
    return stat.transpose(1, 0, 2).reshape(lines, parts * tokens)


def whole(query, key, value, out, output_gradient, log_sum_exp, segment_ids):
    d = HEAD_SIZE
    tokens = query.shape[0]
    parts = lax.axis_size(GROUP)
    outers = lax.axis_size("outer")
    rows = tokens * parts
    heads = query.shape[1] // key.shape[1]
    half = heads // 2
    window = LONGEST
    place = lax.axis_index("outer")

    kv = jnp.concatenate(
        [key.reshape(tokens, parts, d), value.reshape(tokens, parts, d)], axis=2
    ).transpose(1, 0, 2)
    kv = lax.all_to_all(kv, GROUP, 0, 0).reshape(rows, 2 * d)
    delta = jnp.sum(
        (output_gradient.astype(jnp.float32) * out.astype(jnp.float32)).reshape(tokens, -1, d), axis=2
    )
    stat = jnp.stack([log_sum_exp * LOG2E, delta], axis=2).reshape(tokens, parts, 2 * heads).transpose(1, 2, 0)
    query_heads = query.reshape(tokens, parts, heads * d)
    grad_heads = output_gradient.reshape(tokens, parts, heads * d)
    bulk = []
    for n in range(2):
        cut = slice(n * half * d, (n + 1) * half * d)
        sent = packed(
            query_heads[:, :, cut], grad_heads[:, :, cut], stat[:, 2 * half * n : 2 * half * (n + 1)], parts
        )
        bulk.append(lax.all_to_all(sent, GROUP, 0, 0))
    stats = [unpacked_stat(b, tokens, 2 * half) for b in bulk]

    steps = -(-window // rows)
    sizes = [min(rows, window - by * rows) for by in range(steps)]
    arrived = []
    for by in range(1, steps + 1):
        arrived.append(
            lax.ppermute(kv[rows - sizes[by - 1] :], "outer", [(i, i + by) for i in range(outers - by)])
        )
    padded = jnp.concatenate([jnp.full((window,), -1, segment_ids.dtype), segment_ids])
    seg_keys = lax.dynamic_slice_in_dim(padded, place * rows, window + rows, 0)
    seg_query = seg_keys[window:]
    start = jnp.sum((seg_keys[:, None] < seg_query[None, :]).astype(jnp.int32), axis=0)
    low = start[::TILE_Q]
    start = start[None, :]

    smem = pl.BlockSpec(memory_space=pltpu.SMEM)
    vmem = pl.BlockSpec(memory_space=pltpu.VMEM)
    flops = 10 * rows * d * half * 512
    dq_shape = jax.ShapeDtypeStruct((half, d, rows), jnp.float32)
    dq_done = jax.ShapeDtypeStruct((rows, half * d), jnp.bfloat16)
    dkv_shape = jax.ShapeDtypeStruct((rows, 2 * d), jnp.float32)

    def call(kernel, out_shape, scratch, work, *operands):
        return pl.pallas_call(
            kernel,
            out_shape=out_shape,
            in_specs=[smem] + [vmem] * (len(operands) - 1),
            out_specs=(vmem,) * len(out_shape),
            scratch_shapes=scratch,
            cost_estimate=pl.CostEstimate(flops=work, bytes_accessed=1 << 22, transcendentals=0),
        )(*operands)

    dq_near, dkv_near = call(
        functools.partial(early_kernel, tokens, window),
        (dq_shape, dkv_shape),
        [],
        flops,
        *(low, bulk[0], stats[0], start, kv),
    )
    dq_a, dq_far, *dkv_far = call(
        functools.partial(far_kernel, tokens, steps),
        (dq_done, dq_shape) + tuple(jax.ShapeDtypeStruct((size, 2 * d), jnp.bfloat16) for size in sizes),
        [
            pltpu.VMEM((heads, d, rows), jnp.float32),
            pltpu.VMEM((window, 2 * d), jnp.float32),
            pltpu.VMEM((window, 2 * d), jnp.bfloat16),
        ],
        4 * flops,
        *(low, bulk[0], bulk[1], jnp.concatenate(stats, axis=0), start, *arrived, dq_near),
    )
    returned = []
    for by in range(1, steps + 1):
        returned.append(
            lax.ppermute(dkv_far[by - 1], "outer", [(i + by, i) for i in range(outers - by)])
        )
    dq_a = lax.all_to_all(dq_a.reshape(parts, tokens, half * d), GROUP, 0, 0)
    dq_b, dkv = call(
        functools.partial(late_kernel, tokens, window),
        (dq_done, dkv_shape),
        [pltpu.VMEM((half, d, rows), jnp.float32)],
        flops,
        *(low, bulk[1], stats[1], start, kv, dq_far, dkv_near),
    )
    dq_b = lax.all_to_all(dq_b.reshape(parts, tokens, half * d), GROUP, 0, 0)
    for by in range(1, steps + 1):
        part = returned[by - 1].astype(jnp.float32)
        dkv = dkv + jnp.pad(part, ((rows - sizes[by - 1], 0), (0, 0)))
    dkv = lax.all_to_all(dkv.astype(jnp.bfloat16).reshape(parts, tokens, 2 * d), GROUP, 0, 0)
    dkv = dkv.transpose(1, 0, 2)
    return (
        jnp.concatenate([dq_a, dq_b], axis=2).transpose(1, 0, 2).reshape(tokens, -1),
        dkv[:, :, :d].reshape(tokens, -1),
        dkv[:, :, d:].reshape(tokens, -1),
    )


def solution(mesh):
    head = mesh.shape["head"]
    seq = mesh.shape["seq"]

    def run(query, key, value, out, output_gradient, log_sum_exp, segment_ids):
        inner = key.shape[1] // HEAD_SIZE // head
        finer = Mesh(mesh.devices.reshape(seq // inner, inner, head), ("outer", "inner", "head"))
        rows = P(("outer", "inner", "head"), None)
        return jax.shard_map(
            whole,
            mesh=finer,
            in_specs=(rows,) * 6 + (P(),),
            out_specs=(rows,) * 3,
            check_vma=False,
        )(query, key, value, out, output_gradient, log_sum_exp, segment_ids)

    return run
```
